32 devices in a mesh: zero: 2 (over core), model: 16 (over z, y, x).
Axes of the slice: x: 2, y: 2, z: 4, core: 2. Of those that a mesh axis runs over, the one named last changes fastest.
Arguments:
- w_gate: float32 [5120, 13824], P('zero', 'model'), may hold values from -0.125 to 0.125
- first_gate: float32 [5120, 13824], P('zero', 'model'), may hold values from -0.078125 to 0.078125
- second_gate: float32 [5120, 13824], P('zero', 'model'), may hold values from -0.078125 to 0.078125
- w_up: float32 [5120, 13824], P('zero', 'model'), may hold values from -0.125 to 0.125
- first_up: float32 [5120, 13824], P('zero', 'model'), may hold values from -0.078125 to 0.078125
- second_up: float32 [5120, 13824], P('zero', 'model'), may hold values from -0.078125 to 0.078125
- norm_train: float32 [5120], P(('zero', 'model')), may hold values from 0.25 to 1.75
- norm_step: float32 [5120], P(('zero', 'model')), may hold values from -0.3 to 0.3
Outputs:
- ready_gate: bfloat16 [5120, 13824], P(None, 'model')
- ready_up: bfloat16 [5120, 13824], P(None, 'model')
- column_gate: float32 [13824], P('model')
- column_up: float32 [13824], P('model')
- serve_norm: bfloat16 [5120], replicated
- latest_gate: float32 [5120, 13824], P('zero', 'model')
- latest_up: float32 [5120, 13824], P('zero', 'model')
The draws below stay inside these ranges and needn't reach their ends.
All inputs are finite; a program needn't handle non-finite values. Where the reference program divides by a largest or mean magnitude, that divisor is 1e-20 or more.
Results may differ from the reference program's by a relative error of at most 0.001.
Values may be sent and summed in bfloat16 or wider, within the bound.
No kernel may reach another device: no remote copies, remote signals or barrier semaphores. Data moves between devices by JAX's collectives and lax.ppermute only.
A program may use at most 192 MiB of HBM per device.

```python
import jax
import jax.numpy as jnp

D_MODEL = 5120
D_INNER = 13824


def strengthened(result, rng, source, target, parts, factor):
    def block_of(axis_at):
        return (jnp.arange(result.shape[axis_at]) // (result.shape[axis_at] // parts)).reshape((-1,) + (1,) * (result.ndim - 1 - axis_at))

    first = jax.random.permutation(rng, parts)[block_of(target)]
    second = (block_of(target) + parts // 2) % parts
    return jnp.where((block_of(source) == first) | (block_of(source) == second), factor * result, result)


def block_scale(stream_key, dims, split, smallest, largest):
    loudness, own = 1.0, jax.random.fold_in(stream_key, 6)
    for position, blocks in split:
        draws = jnp.exp(jax.random.uniform(jax.random.fold_in(own, position), (blocks,), jnp.float32, smallest / len(split), largest / len(split)))
        loudness = loudness * jnp.repeat(draws, dims[position] // blocks).reshape([-1 if axis == position else 1 for axis in range(len(dims))])
    return loudness


def scatter_about(stream_key, shape, spread, reach, pieces=(), dtype=jnp.bfloat16):
    loudness = block_scale(stream_key, shape, pieces, -0.22, 0.18) if pieces else 1.0
    values = jax.random.normal(stream_key, shape, jnp.float32) * spread * loudness
    return jnp.minimum(jnp.maximum(values, -reach), reach).astype(dtype)


def gaussian_with(key, shape, spread, most, split, heavy, kind=jnp.bfloat16):
    values = spread * jax.random.normal(key, shape, jnp.float32)
    if split:
        values = values * block_scale(key, shape, split, -0.22, 0.18)
    return jnp.clip(strengthened(values, jax.random.fold_in(key, 3), *heavy), -most, most).astype(kind)


def setup_inputs(seed: int = 0) -> dict:
    splits = jax.random.split(jax.random.key(seed), 9)
    w_gate = gaussian_with(splits[0], (D_MODEL, D_INNER), D_MODEL ** -0.5, 0.125, ((0, 2), (1, 16)), (0, 1, 16, 2.0), jnp.float32)
    first_gate = scatter_about(splits[1], (D_MODEL, D_INNER), D_MODEL ** -0.5, 0.078125, ((0, 2), (1, 16)), jnp.float32)
    second_gate = scatter_about(splits[2], (D_MODEL, D_INNER), D_MODEL ** -0.5, 0.078125, ((0, 2), (1, 16)), jnp.float32)
    w_up = gaussian_with(splits[3], (D_MODEL, D_INNER), D_MODEL ** -0.5, 0.125, ((0, 2), (1, 16)), (0, 1, 16, 2.0), jnp.float32)
    first_up = scatter_about(splits[4], (D_MODEL, D_INNER), D_MODEL ** -0.5, 0.078125, ((0, 2), (1, 16)), jnp.float32)
    second_up = scatter_about(splits[5], (D_MODEL, D_INNER), D_MODEL ** -0.5, 0.078125, ((0, 2), (1, 16)), jnp.float32)
    norm_train = jnp.clip(1.0 + 0.15 * jax.random.normal(splits[6], (D_MODEL,), jnp.float32), 0.25, 1.75)
    norm_step = jnp.clip(jax.random.uniform(splits[7], (D_MODEL,), jnp.float32, -0.3, 0.3) * block_scale(splits[7], (D_MODEL,), ((0, 32),), -0.4, 0.0), -0.3, 0.3)
    return dict(w_gate=w_gate, first_gate=first_gate, second_gate=second_gate, w_up=w_up, first_up=first_up, second_up=second_up, norm_train=norm_train, norm_step=norm_step)


learn_rate = 0.25
hold_rate = 0.8


def reference(w_gate, first_gate, second_gate, w_up, first_up, second_up, norm_train, norm_step):
    hold_gate = hold_rate * first_gate + second_gate
    latest_gate = w_gate - learn_rate * hold_gate
    hold_up = hold_rate * first_up + second_up
    latest_up = w_up - learn_rate * hold_up
    column_gate = jnp.max(jnp.abs(latest_gate), axis=0)
    ready_gate = (latest_gate / column_gate).astype(jnp.bfloat16)
    column_up = jnp.max(jnp.abs(latest_up), axis=0)
    ready_up = (latest_up / column_up).astype(jnp.bfloat16)
    serve_norm = (norm_train + norm_step).astype(jnp.bfloat16)
    return ready_gate, ready_up, column_gate, column_up, serve_norm, latest_gate, latest_up
```

```python
import functools

import jax
import jax.numpy as jnp
from jax import lax
from jax.experimental import pallas as pl
from jax.experimental.pallas import tpu as pltpu
from jax.sharding import PartitionSpec as P


learn_rate = 0.25
hold_rate = 0.8

LANES = 128
GROUP = 8
PARTS = ((0, 0.3), (0, 0.4), (0, 0.3), (1, 0.45), (1, 0.3), (1, 0.25))
STAGES = (
    ((0,), (), ()),
    ((1,), (), ()),
    ((2,), (0,), ()),
    ((3,), (1,), ()),
    ((4,), (2,), (0,)),
    ((5,), (3,), (1,)),
    ((), (4,), (2,)),
    ((), (5,), (3,)),
    ((), (), (4, 5)),
)
BLOCK = 32
DEPTH = 8
SPARE = 3 << 20


def up_to(value, unit):
    return -(-value // unit) * unit


def cut(columns):
    parts, at, total = [], [0, 0], [0.0, 0.0]
    for k, (matrix, share) in enumerate(PARTS):
        total[matrix] += share
        last = all(other != matrix for other, _ in PARTS[k + 1 :])
        end = columns if last else min(round(total[matrix] * columns / LANES) * LANES, columns)
        parts.append((matrix, at[matrix], end - at[matrix]))
        at[matrix] = end
    return parts


def blocks_of(first, size):
    return [(at, min(BLOCK, first + size - at)) for at in range(first, first + size, BLOCK)]


def stream_of(parts):
    return [(p, matrix, first, some) for p, (matrix, at, size) in enumerate(parts) for first, some in blocks_of(at, size)]


def rows_of(first, g):
    return pl.ds(pl.multiple_of(first + g * GROUP, GROUP), GROUP)


def compute(w, f, s, latest, top_out, at, some, rows):
    @pl.loop(0, some // GROUP)
    def _(g):
        here, there = rows_of(0, g), rows_of(at, g)
        top = None
        for lane in range(0, rows, LANES):
            lanes = pl.ds(lane, LANES)
            value = w[here, lanes] - learn_rate * (hold_rate * f[here, lanes] + s[here, lanes])
            latest[there, lanes] = value
            top = jnp.abs(value) if top is None else jnp.maximum(top, jnp.abs(value))
        top_out[there, :] = jnp.broadcast_to(jnp.max(top, axis=1, keepdims=True), (GROUP, LANES))


def stage_kernel(plan, n, rows, stream, fetched, names, *refs):
    r = dict(zip(names, refs, strict=True))
    a, b, c = plan
    parts_at = {p: at for p, _, at, _ in a}
    me = lax.axis_index("zero")
    pending = []

    def start(*copy):
        copy = pltpu.make_async_copy(*copy)
        copy.start()
        pending.append(copy)

    for p, matrix, at, size in c:
        for s in range(n - 1):
            source = lax.rem(me + n - (s + 1), n)
            place = pl.ds(pl.multiple_of(source * rows, LANES), rows)
            start(r["arrived", p, s], r["ready", matrix].at[pl.ds(at, size), place], r["c_sem", p].at[s])

    wanted = {}

    def read(i):
        _, matrix, first, some = stream[i]
        wanted[i] = [
            pltpu.make_async_copy(
                r["x", matrix, k].at[pl.ds(first, some), :],
                r["ring"].at[k, i % DEPTH, pl.ds(0, some), :],
                r["in_sem"].at[k, i % DEPTH],
            )
            for k in range(3)
        ]
        for copy in wanted[i]:
            copy.start()

    computed, ready, end = fetched
    for i in range(ready, min(computed + DEPTH, len(stream))):
        read(i)

    r["token"][...] = jnp.zeros((GROUP, LANES), jnp.float32)
    if "gain" in r:
        r["gain"][...] = r["gain_in"][...] + r["gain_near"][...]

    for p, matrix, at, size in b:
        own = pl.ds(pl.multiple_of(me * rows, LANES), rows)
        for i, (first, some) in enumerate(blocks_of(0, size)):

            @pl.loop(0, some // GROUP)
            def _(g):
                here = rows_of(first, g)
                top = r["top_in", p][here, :]
                for s in range(n - 1):
                    top = jnp.maximum(top, r["top_near", p, s][here, :])
                r["column_top"][here, :] = top
                scale = 1.0 / top
                for lane in range(0, rows, LANES):
                    lanes = pl.ds(lane, LANES)
                    r["send", p][here, lanes] = (r["latest_in", p][here, lanes] * scale).astype(jnp.bfloat16)

            start(
                r["send", p].at[pl.ds(first, some), :],
                r["ready", matrix].at[pl.ds(at + first, some), own],
                r["b_sem", p].at[i],
            )
        if ("column_in", matrix) in r:
            r["column", matrix][pl.ds(0, at)] = r["column_in", matrix][pl.ds(0, at)]
        for first in range(0, size, LANES):
            some = min(LANES, size - first)
            line = r["column_top"][pl.ds(first, LANES), :].T[0, :]
            r["column", matrix][pl.ds(at + first, some)] = line[:some]

    for i in range(computed, end):
        p, matrix, first, some = stream[i]
        at = first - parts_at[p]
        for copy in wanted.pop(i, ()):
            copy.wait()
        ring = [r["ring"].at[k, i % DEPTH] for k in range(3)]
        compute(*ring, r["latest_out", p], r["top_out", p], at, some, rows)
        start(
            r["latest_out", p].at[pl.ds(at, some), :],
            r["latest", matrix].at[pl.ds(first, some), :],
            r["a_sem"].at[i - computed],
        )
        if i + DEPTH < len(stream):
            read(i + DEPTH)
    for copies in wanted.values():
        for copy in copies:
            copy.wait()
    for copy in pending:
        copy.wait()


def local(n, w_gate, first_gate, second_gate, w_up, first_up, second_up, norm_train, norm_step):
    columns, rows = w_gate.shape[1], w_gate.shape[0]
    parts = cut(columns)
    sources = [[x.T for x in (w_gate, first_gate, second_gate)], [x.T for x in (w_up, first_up, second_up)]]
    perms = [[(i, (i + s) % n) for i in range(n)] for s in range(1, n)]
    held = {}
    state = [dict() for _ in parts]
    any_spec = pl.BlockSpec(memory_space=pl.ANY)
    v_spec = pl.BlockSpec(memory_space=pltpu.VMEM)
    stream = stream_of(parts)
    computed = ready = 0

    share = (norm_train + norm_step).astype(jnp.bfloat16)
    model = lax.axis_size("model")
    place = (lax.axis_index("zero") * model + lax.axis_index("model")) * share.shape[0]
    zeros = jnp.zeros((n * model * share.shape[0],), jnp.bfloat16)
    held["gain"] = lax.dynamic_update_slice(zeros, share, (place,)).reshape(-1, LANES)
    hops = [
        (axis, [(i, i ^ (1 << k)) for i in range(size)])
        for axis, size in (("model", model), ("zero", n))
        for k in range(size.bit_length() - 1)
    ]

    def hop(number):
        if hops and "near" not in held:
            axis, perm = hops.pop(0)
            held["near"] = lax.ppermute(held["gain"], axis, perm)
            held["due"] = min(number + 2, len(STAGES) - 1)

    def stage(number, a, b, c):
        nonlocal computed, ready
        plan = [[(p, *parts[p]) for p in ps if parts[p][2]] for ps in (a, b, c)]
        ins, outs, scratch, alias = {}, {}, {}, {}
        moved = 0
        latest_spec = (pltpu.HBM((columns, rows), jnp.float32), any_spec)
        ready_spec = (pltpu.HBM((columns, n * rows), jnp.bfloat16), any_spec)
        for p, matrix, at, size in plan[0]:
            outs["latest", matrix] = latest_spec
            outs["top_out", p] = (pltpu.VMEM((size, LANES), jnp.float32), v_spec)
            outs["latest_out", p] = (pltpu.VMEM((size, rows), jnp.float32), v_spec)
            moved += 16 * size * rows
        end = computed + sum(1 for block in stream if block[0] in [part[0] for part in plan[0]])
        fetched = (computed, ready, end)
        if end > computed:
            scratch["a_sem"] = pltpu.SemaphoreType.DMA((end - computed,))
            for matrix in sorted({stream[i][1] for i in range(ready, min(end + DEPTH, len(stream)))}):
                for k in range(3):
                    ins["x", matrix, k] = (sources[matrix][k], any_spec)
            if "ring" in held:
                ins["ring_in"] = (held["ring"], v_spec)
                alias["ring_in"] = "ring"
            outs["ring"] = (pltpu.VMEM((3, DEPTH, BLOCK, rows), jnp.float32), v_spec)
            scratch["in_sem"] = pltpu.SemaphoreType.DMA((3, DEPTH))
            computed, ready = end, min(end + DEPTH, len(stream))
        else:
            fetched = (0, len(stream), 0)
        for p, matrix, at, size in plan[1]:
            ins["latest_in", p] = (state[p]["latest"], v_spec)
            ins["top_in", p] = (state[p]["top"], v_spec)
            for s, x in enumerate(state[p]["tops"]):
                ins["top_near", p, s] = (x, v_spec)
            outs["ready", matrix] = ready_spec
            outs["send", p] = (pltpu.VMEM((size, rows), jnp.bfloat16), v_spec)
            if ("column", matrix) in held:
                ins["column_in", matrix] = (held["column", matrix], v_spec)
            space = pltpu.HBM if at + size == columns else pltpu.VMEM
            outs["column", matrix] = (space((columns,), jnp.float32), v_spec)
            scratch["column_top"] = pltpu.VMEM((up_to(size, LANES), LANES), jnp.float32)
            scratch["b_sem", p] = pltpu.SemaphoreType.DMA((len(blocks_of(0, size)),))
            moved += 4 * size * rows
        for p, matrix, at, size in plan[2]:
            for s, x in enumerate(state[p]["arrived"]):
                ins["arrived", p, s] = (x, v_spec)
            if number + 1 < len(STAGES):
                ins["sent", p] = (state[p]["send"], v_spec)
            outs["ready", matrix] = ready_spec
            scratch["c_sem", p] = pltpu.SemaphoreType.DMA((n - 1,))
            moved += 2 * size * rows * (n - 1)
        if "token" in held:
            ins["token_in"] = (held["token"], v_spec)
        if "near" in held and number == held["due"]:
            ins["gain_in"] = (held["gain"], v_spec)
            ins["gain_near"] = (held.pop("near"), v_spec)
            space = pltpu.VMEM if hops else pltpu.HBM
            outs["gain"] = (space(held["gain"].shape, jnp.bfloat16), v_spec)
        outs["token"] = (pltpu.VMEM((GROUP, LANES), jnp.float32), v_spec)
        for name in outs:
            if name[0] in ("latest", "ready") and name in held:
                ins["in", name] = (held[name], any_spec)
                alias["in", name] = name
        order_in, order_out = list(ins), list(outs)
        results = pl.pallas_call(
            functools.partial(stage_kernel, plan, n, rows, stream, fetched, [*ins, *outs, *scratch]),
            out_shape=[o[0] for o in outs.values()],
            in_specs=[i[1] for i in ins.values()],
            out_specs=[o[1] for o in outs.values()],
            scratch_shapes=list(scratch.values()),
            input_output_aliases={order_in.index(i): order_out.index(o) for i, o in alias.items()},
            cost_estimate=pl.CostEstimate(flops=300 * moved, bytes_accessed=moved, transcendentals=0),
            compiler_params=pltpu.CompilerParams(vmem_limit_bytes=SPARE),
        )(
            *[
                pltpu.with_memory_space_constraint(x, pltpu.VMEM if spec is v_spec else pltpu.HBM)
                for x, spec in ins.values()
            ]
        )
        results = dict(zip(outs, results))
        for name, x in results.items():
            if name[0] in ("latest", "ready", "column") or name in ("token", "ring", "gain"):
                held[name] = x
        for p, matrix, _, _ in plan[0]:
            state[p]["latest"] = results.get(("latest_out", p))
            state[p]["top"] = results["top_out", p]
            state[p]["tops"] = [lax.ppermute(results["top_out", p], "zero", perm) for perm in perms]
        for p, _, _, _ in plan[1]:
            state[p]["send"] = results["send", p]
            state[p]["arrived"] = [lax.ppermute(results["send", p], "zero", perm) for perm in perms]

    hop(-1)
    for number, (a, b, c) in enumerate(STAGES):
        stage(number, a, b, c)
        hop(number)
    return (
        held["ready", 0].T,
        held["ready", 1].T,
        held["column", 0],
        held["column", 1],
        held["gain"].reshape(-1),
        held["latest", 0].T,
        held["latest", 1].T,
    )


def solution(mesh):
    n = mesh.shape["zero"]
    spec = P("zero", "model")
    specs = dict(
        mesh=mesh,
        in_specs=(spec,) * 6 + (P(("zero", "model")),) * 2,
        out_specs=(P(None, "model"), P(None, "model"), P("model"), P("model"), P(), spec, spec),
        check_vma=False,
    )
    return jax.shard_map(functools.partial(local, n), **specs)
```

```python
import functools

import jax
import jax.numpy as jnp
from jax import lax
from jax.experimental import pallas as pl
from jax.experimental.pallas import tpu as pltpu
from jax.sharding import PartitionSpec as P


learn_rate = 0.25
hold_rate = 0.8

LANES = 128
GROUP = 8
PARTS = ((0, 1.0), (1, 0.3), (1, 0.3), (1, 0.4))
STAGES = (
    ((0,), (), (), ()),
    ((1,), (), (), ()),
    ((2,), (0,), (), ()),
    ((3,), (1,), (), ()),
    ((), (2, 3), (), ()),
    ((), (), (), ()),
    ((), (), (0, 1), ()),
    ((), (), (), ()),
    ((), (), (2, 3), ()),
)
HOPS = ((-1, 1), (1, 3), (3, 5), (5, 7), (7, 8))
BLOCK = 32
DEPTH = 5
SPARE = 3 << 20


def up_to(value, unit):
    return -(-value // unit) * unit


def cut(columns):
    parts, at, total = [], [0, 0], [0.0, 0.0]
    for k, (matrix, share) in enumerate(PARTS):
        total[matrix] += share
        last = all(other != matrix for other, _ in PARTS[k + 1 :])
        end = columns if last else min(round(total[matrix] * columns / LANES) * LANES, columns)
        parts.append((matrix, at[matrix], end - at[matrix]))
        at[matrix] = end
    return parts


def blocks_of(first, size):
    return [(at, min(BLOCK, first + size - at)) for at in range(first, first + size, BLOCK)]


def stream_of(parts):
    return [(p, matrix, first, some) for p, (matrix, at, size) in enumerate(parts) for first, some in blocks_of(at, size)]


def rows_of(first, g):
    return pl.ds(pl.multiple_of(first + g * GROUP, GROUP), GROUP)


def compute(w, f, s, latest, top_out, at, some, rows):
    @pl.loop(0, some // GROUP)
    def _(g):
        here, there = rows_of(0, g), rows_of(at, g)
        top = None
        for lane in range(0, rows, LANES):
            lanes = pl.ds(lane, LANES)
            value = w[here, lanes] - learn_rate * (hold_rate * f[here, lanes] + s[here, lanes])
            latest[there, lanes] = value
            top = jnp.abs(value) if top is None else jnp.maximum(top, jnp.abs(value))
        top_out[there, :] = jnp.broadcast_to(jnp.max(top, axis=1, keepdims=True), (GROUP, LANES))


def stage_kernel(plan, n, rows, stream, fetched, names, *refs):
    r = dict(zip(names, refs, strict=True))
    a, b, c, w = plan
    late = [p for stage in STAGES for p in stage[3]]
    parts_at = {p: at for p, _, at, _ in a}
    me = lax.axis_index("zero")
    pending = []

    def start(*copy):
        pltpu.make_async_copy(*copy).start()

    def wait_at_end(*copy):
        pending.append(pltpu.make_async_copy(*copy))

    for p, matrix, at, size in c:
        for s in range(n - 1):
            source = lax.rem(me + n - (s + 1), n)
            place = pl.ds(pl.multiple_of(source * rows, LANES), rows)
            copy = (r["arrived", p, s], r["ready", matrix].at[pl.ds(at, size), place], r["c_sem", p].at[s])
            wait_at_end(*copy)
            for first, some in blocks_of(0, size):
                start(copy[0].at[pl.ds(first, some), :], r["ready", matrix].at[pl.ds(at + first, some), place], copy[2])

    wanted = {}

    def read(i):
        _, matrix, first, some = stream[i]
        slot = i % DEPTH
        for k in range(3):
            pltpu.make_async_copy(
                r["x", matrix, k].at[pl.ds(first, some), :],
                r["ring"].at[slot, k, pl.ds(0, some), :],
                r["in_sem"].at[slot],
            ).start()
        block = r["ring"].at[slot, :, pl.ds(0, some), :]
        wanted[i] = pltpu.make_async_copy(block, block, r["in_sem"].at[slot])

    computed, ready, end = fetched
    for i in range(ready, min(computed + DEPTH, len(stream))):
        read(i)

    def compute_blocks(computed, end):
        for i in range(computed, end):
            p, matrix, first, some = stream[i]
            at = first - parts_at[p]
            if i in wanted:
                wanted.pop(i).wait()
            ring = [r["ring"].at[i % DEPTH, k] for k in range(3)]
            compute(*ring, r["latest_out", p], r["top_out", p], at, some, rows)
            if p not in late:
                start(
                    r["latest_out", p].at[pl.ds(at, some), :],
                    r["latest", matrix].at[pl.ds(first, some), :],
                    r["a_sem", p],
                )
            if i + DEPTH < len(stream):
                read(i + DEPTH)

    at_once = min(ready, end)
    compute_blocks(computed, at_once)
    r["token"][...] = jnp.zeros((GROUP, LANES), jnp.float32)
    if "gain" in r:
        r["gain"][...] = r["gain_in"][...] + r["gain_near"][...]

    for p, matrix, at, size in b:
        own = pl.ds(pl.multiple_of(me * rows, LANES), rows)
        for first, some in blocks_of(0, size):

            @pl.loop(0, some // GROUP)
            def _(g):
                here = rows_of(first, g)
                top = r["top_in", p][here, :]
                for s in range(n - 1):
                    top = jnp.maximum(top, r["top_near", p, s][here, :])
                r["column_top"][here, :] = top
                scale = 1.0 / top
                for lane in range(0, rows, LANES):
                    lanes = pl.ds(lane, LANES)
                    r["send", p][here, lanes] = (r["latest_in", p][here, lanes] * scale).astype(jnp.bfloat16)

            start(
                r["send", p].at[pl.ds(first, some), :],
                r["ready", matrix].at[pl.ds(at + first, some), own],
                r["b_sem", p],
            )
        wait_at_end(r["send", p], r["ready", matrix].at[pl.ds(at, size), own], r["b_sem", p])
        if ("column_in", matrix) in r and all(at <= other[2] for other in b if other[1] == matrix):
            r["column", matrix][pl.ds(0, at)] = r["column_in", matrix][pl.ds(0, at)]
        for first in range(0, size, LANES):
            some = min(LANES, size - first)
            line = r["column_top"][pl.ds(first, LANES), :].T[0, :]
            r["column", matrix][pl.ds(at + first, some)] = line[:some]

    compute_blocks(max(computed, at_once), end)
    for p, matrix, at, size in w:
        for first, some in blocks_of(0, size):
            start(
                r["latest_late", p].at[pl.ds(first, some), :],
                r["latest", matrix].at[pl.ds(at + first, some), :],
                r["a_sem", p],
            )
        wait_at_end(r["latest_late", p], r["latest", matrix].at[pl.ds(at, size), :], r["a_sem", p])
    for p, matrix, at, size in [part for part in a if part[0] not in late]:
        wait_at_end(r["latest_out", p], r["latest", matrix].at[pl.ds(at, size), :], r["a_sem", p])
    for copy in wanted.values():
        copy.wait()
    for copy in pending:
        copy.wait()


def local(n, w_gate, first_gate, second_gate, w_up, first_up, second_up, norm_train, norm_step):
    columns, rows = w_gate.shape[1], w_gate.shape[0]
    parts = cut(columns)
    sources = [[x.T for x in (w_gate, first_gate, second_gate)], [x.T for x in (w_up, first_up, second_up)]]
    perms = [[(i, (i + s) % n) for i in range(n)] for s in range(1, n)]
    held = {}
    state = [dict() for _ in parts]
    any_spec = pl.BlockSpec(memory_space=pl.ANY)
    v_spec = pl.BlockSpec(memory_space=pltpu.VMEM)
    stream = stream_of(parts)
    computed = ready = 0

    share = (norm_train + norm_step).astype(jnp.bfloat16)
    model = lax.axis_size("model")
    place = (lax.axis_index("zero") * model + lax.axis_index("model")) * share.shape[0]
    zeros = jnp.zeros((n * model * share.shape[0],), jnp.bfloat16)
    held["gain"] = lax.dynamic_update_slice(zeros, share, (place,)).reshape(-1, LANES)
    hops = [
        (axis, [(i, i ^ (1 << k)) for i in range(size)])
        for axis, size in (("model", model), ("zero", n))
        for k in range(size.bit_length() - 1)
    ]

    def hop(number):
        for begin, due in HOPS:
            if begin == number and hops:
                axis, perm = hops.pop(0)
                held["near"] = lax.ppermute(held["gain"], axis, perm)
                held["due"] = due

    def stage(number, *lists):
        nonlocal computed, ready
        plan = [[(p, *parts[p]) for p in ps if parts[p][2]] for ps in lists]
        late = [p for stage in STAGES for p in stage[3]]
        ins, outs, scratch, alias = {}, {}, {}, {}
        moved = 0
        latest_spec = (pltpu.HBM((columns, rows), jnp.float32), any_spec)
        ready_spec = (pltpu.HBM((columns, n * rows), jnp.bfloat16), any_spec)
        for p, matrix, at, size in plan[0]:
            if p not in late:
                outs["latest", matrix] = latest_spec
                scratch["a_sem", p] = pltpu.SemaphoreType.DMA
            outs["top_out", p] = (pltpu.VMEM((size, LANES), jnp.float32), v_spec)
            outs["latest_out", p] = (pltpu.VMEM((size, rows), jnp.float32), v_spec)
            moved += 16 * size * rows
        end = computed + sum(1 for block in stream if block[0] in [part[0] for part in plan[0]])
        fetched = (computed, ready, end)
        if end > computed:
            for matrix in sorted({stream[i][1] for i in range(ready, min(end + DEPTH, len(stream)))}):
                for k in range(3):
                    ins["x", matrix, k] = (sources[matrix][k], any_spec)
            if "ring" in held:
                ins["ring_in"] = (held["ring"], v_spec)
                alias["ring_in"] = "ring"
            outs["ring"] = (pltpu.VMEM((DEPTH, 3, BLOCK, rows), jnp.float32), v_spec)
            scratch["in_sem"] = pltpu.SemaphoreType.DMA((DEPTH,))
            computed, ready = end, min(end + DEPTH, len(stream))
        else:
            fetched = (0, len(stream), 0)
        for p, matrix, at, size in plan[1]:
            ins["latest_in", p] = (state[p]["latest"], v_spec)
            ins["top_in", p] = (state[p]["top"], v_spec)
            for s, x in enumerate(state[p]["tops"]):
                ins["top_near", p, s] = (x, v_spec)
            outs["ready", matrix] = ready_spec
            outs["send", p] = (pltpu.VMEM((size, rows), jnp.bfloat16), v_spec)
            if ("column", matrix) in held:
                ins["column_in", matrix] = (held["column", matrix], v_spec)
            space = pltpu.HBM if at + size == columns else pltpu.VMEM
            outs["column", matrix] = (space((columns,), jnp.float32), v_spec)
            most = max(up_to(part[3], LANES) for part in plan[1])
            scratch["column_top"] = pltpu.VMEM((most, LANES), jnp.float32)
            scratch["b_sem", p] = pltpu.SemaphoreType.DMA
            moved += 4 * size * rows
        for p, matrix, at, size in plan[2]:
            for s, x in enumerate(state[p]["arrived"]):
                ins["arrived", p, s] = (x, v_spec)
            if number + 1 < len(STAGES):
                ins["sent", p] = (state[p]["send"], v_spec)
            outs["ready", matrix] = ready_spec
            scratch["c_sem", p] = pltpu.SemaphoreType.DMA((n - 1,))
            moved += 2 * size * rows * (n - 1)
        for p, matrix, at, size in plan[3]:
            ins["latest_late", p] = (state[p]["latest"], v_spec)
            outs["latest", matrix] = latest_spec
            scratch["a_sem", p] = pltpu.SemaphoreType.DMA
            moved += 4 * size * rows
        if "token" in held:
            ins["token_in"] = (held["token"], v_spec)
        if "near" in held and number == held["due"]:
            ins["gain_in"] = (held["gain"], v_spec)
            ins["gain_near"] = (held.pop("near"), v_spec)
            space = pltpu.VMEM if hops else pltpu.HBM
            outs["gain"] = (space(held["gain"].shape, jnp.bfloat16), v_spec)
        outs["token"] = (pltpu.VMEM((GROUP, LANES), jnp.float32), v_spec)
        for name in outs:
            if name[0] in ("latest", "ready") and name in held:
                ins["in", name] = (held[name], any_spec)
                alias["in", name] = name
        order_in, order_out = list(ins), list(outs)
        results = pl.pallas_call(
            functools.partial(stage_kernel, plan, n, rows, stream, fetched, [*ins, *outs, *scratch]),
            out_shape=[o[0] for o in outs.values()],
            in_specs=[i[1] for i in ins.values()],
            out_specs=[o[1] for o in outs.values()],
            scratch_shapes=list(scratch.values()),
            input_output_aliases={order_in.index(i): order_out.index(o) for i, o in alias.items()},
            cost_estimate=pl.CostEstimate(flops=300 * moved, bytes_accessed=moved, transcendentals=0),
            compiler_params=pltpu.CompilerParams(vmem_limit_bytes=SPARE),
        )(
            *[
                pltpu.with_memory_space_constraint(x, pltpu.VMEM if spec is v_spec else pltpu.HBM)
                for x, spec in ins.values()
            ]
        )
        results = dict(zip(outs, results))
        for name, x in results.items():
            if name[0] in ("latest", "ready", "column") or name in ("token", "ring", "gain"):
                held[name] = x
        for p, matrix, _, _ in plan[0]:
            state[p]["latest"] = results.get(("latest_out", p))
            state[p]["top"] = results["top_out", p]
            state[p]["tops"] = [lax.ppermute(results["top_out", p], "zero", perm) for perm in perms]
        for p, _, _, _ in plan[1]:
            state[p]["send"] = results["send", p]
            state[p]["arrived"] = [lax.ppermute(results["send", p], "zero", perm) for perm in perms]

    hop(-1)
    for number, lists in enumerate(STAGES):
        stage(number, *lists)
        hop(number)
    while hops:
        axis, perm = hops.pop(0)
        held["gain"] = held["gain"] + lax.ppermute(held["gain"], axis, perm)
    return (
        held["ready", 0].T,
        held["ready", 1].T,
        held["column", 0],
        held["column", 1],
        held["gain"].reshape(-1),
        held["latest", 0].T,
        held["latest", 1].T,
    )


def solution(mesh):
    n = mesh.shape["zero"]
    spec = P("zero", "model")
    specs = dict(
        mesh=mesh,
        in_specs=(spec,) * 6 + (P(("zero", "model")),) * 2,
        out_specs=(P(None, "model"), P(None, "model"), P("model"), P("model"), P(), spec, spec),
        check_vma=False,
    )
    return jax.shard_map(functools.partial(local, n), **specs)
```

```python
import functools
import math

import jax
import jax.numpy as jnp
from jax import lax
from jax.experimental import pallas as pl
from jax.experimental.pallas import tpu as pltpu
from jax.sharding import PartitionSpec as P


learn_rate = 0.25
hold_rate = 0.8

LANES = 128
GROUP = 8
PARTS = ((0, 1.0), (1, 0.3), (1, 0.3), (1, 0.4))
STAGES = (
    ((0,), (), (), ()),
    ((1,), (), (), ()),
    ((), (), (), ()),
    ((2,), (0,), (), ()),
    ((), (), (), ()),
    ((3,), (1,), (), ()),
    ((), (), (), ()),
    ((), (2, 3), (), ()),
    ((), (), (), ()),
    ((), (), (0, 1), ()),
    ((), (), (2, 3), ()),
)
HOPS = ((0, 2), (2, 4), (4, 6), (6, 8), (8, 10))
BLOCK = 32
DEPTH = 5
SPARE = 3 << 20


def up_to(value, unit):
    return -(-value // unit) * unit


def cut(columns):
    parts, at, total = [], [0, 0], [0.0, 0.0]
    for k, (matrix, share) in enumerate(PARTS):
        total[matrix] += share
        last = all(other != matrix for other, _ in PARTS[k + 1 :])
        end = columns if last else min(round(total[matrix] * columns / LANES) * LANES, columns)
        parts.append((matrix, at[matrix], end - at[matrix]))
        at[matrix] = end
    return parts


def blocks_of(first, size):
    return [(at, min(BLOCK, first + size - at)) for at in range(first, first + size, BLOCK)]


def stream_of(parts):
    return [(p, matrix, first, some) for p, (matrix, at, size) in enumerate(parts) for first, some in blocks_of(at, size)]


def rows_of(first, g):
    return pl.ds(pl.multiple_of(first + g * GROUP, GROUP), GROUP)


def compute(w, f, s, latest, top_out, at, some, rows):
    @pl.loop(0, some // GROUP)
    def _(g):
        here, there = rows_of(0, g), rows_of(at, g)
        top = None
        for lane in range(0, rows, LANES):
            lanes = pl.ds(lane, LANES)
            value = w[here, lanes] - learn_rate * (hold_rate * f[here, lanes] + s[here, lanes])
            latest[there, lanes] = value
            top = jnp.abs(value) if top is None else jnp.maximum(top, jnp.abs(value))
        top_out[there, :] = jnp.broadcast_to(jnp.max(top, axis=1, keepdims=True), (GROUP, LANES))


def stage_kernel(plan, n, rows, stream, fetched, names, *refs):
    r = dict(zip(names, refs, strict=True))
    a, b, c, w = plan
    late = [p for stage in STAGES for p in stage[3]]
    parts_at = {p: at for p, _, at, _ in a}
    me = lax.axis_index("zero")
    pending = []

    def start(*copy):
        pltpu.make_async_copy(*copy).start()

    def wait_at_end(*copy):
        pending.append(pltpu.make_async_copy(*copy))

    for p, matrix, at, size in c:
        for s in range(n - 1):
            source = lax.rem(me + n - (s + 1), n)
            place = pl.ds(pl.multiple_of(source * rows, LANES), rows)
            copy = (r["arrived", p, s], r["ready", matrix].at[pl.ds(at, size), place], r["c_sem", p].at[s])
            wait_at_end(*copy)
            for first, some in blocks_of(0, size):
                start(copy[0].at[pl.ds(first, some), :], r["ready", matrix].at[pl.ds(at + first, some), place], copy[2])

    if ("norm", 0) in r:
        norms = [
            pltpu.make_async_copy(r["norm", k], r["norm"].at[k], r["norm_sem"].at[k])
            for k in range(2)
        ]
        for copy in norms:
            copy.start()
    wanted = {}

    def read(i):
        _, matrix, first, some = stream[i]
        slot = i % DEPTH
        for k in range(3):
            pltpu.make_async_copy(
                r["x", matrix, k].at[pl.ds(first, some), :],
                r["ring"].at[slot, k, pl.ds(0, some), :],
                r["in_sem"].at[slot],
            ).start()
        block = r["ring"].at[slot, :, pl.ds(0, some), :]
        wanted[i] = pltpu.make_async_copy(block, block, r["in_sem"].at[slot])

    computed, ready, end = fetched
    for i in range(ready, min(computed + DEPTH, len(stream))):
        read(i)

    def compute_blocks(computed, end):
        for i in range(computed, end):
            p, matrix, first, some = stream[i]
            at = first - parts_at[p]
            if i in wanted:
                wanted.pop(i).wait()
            ring = [r["ring"].at[i % DEPTH, k] for k in range(3)]
            compute(*ring, r["latest_out", p], r["top_out", p], at, some, rows)
            if p not in late:
                start(
                    r["latest_out", p].at[pl.ds(at, some), :],
                    r["latest", matrix].at[pl.ds(first, some), :],
                    r["a_sem", p],
                )
            if i + DEPTH < len(stream):
                read(i + DEPTH)

    at_once = min(ready, end)
    compute_blocks(computed, at_once)
    r["token"][...] = jnp.zeros((GROUP, LANES), jnp.float32)
    if "gain_in" in r:
        r["gain"][...] = r["gain_in"][...] + r["gain_near"][...]

    for p, matrix, at, size in b:
        own = pl.ds(pl.multiple_of(me * rows, LANES), rows)
        for first, some in blocks_of(0, size):

            @pl.loop(0, some // GROUP)
            def _(g):
                here = rows_of(first, g)
                top = r["top_in", p][here, :]
                for s in range(n - 1):
                    top = jnp.maximum(top, r["top_near", p, s][here, :])
                r["column_top"][here, :] = top
                scale = 1.0 / top
                for lane in range(0, rows, LANES):
                    lanes = pl.ds(lane, LANES)
                    r["send", p][here, lanes] = (r["latest_in", p][here, lanes] * scale).astype(jnp.bfloat16)

            start(
                r["send", p].at[pl.ds(first, some), :],
                r["ready", matrix].at[pl.ds(at + first, some), own],
                r["b_sem", p],
            )
        wait_at_end(r["send", p], r["ready", matrix].at[pl.ds(at, size), own], r["b_sem", p])
        if ("column_in", matrix) in r and all(at <= other[2] for other in b if other[1] == matrix):
            r["column", matrix][pl.ds(0, at)] = r["column_in", matrix][pl.ds(0, at)]
        for first in range(0, size, LANES):
            some = min(LANES, size - first)
            line = r["column_top"][pl.ds(first, LANES), :].T[0, :]
            r["column", matrix][pl.ds(at + first, some)] = line[:some]

    compute_blocks(max(computed, at_once), end)
    if ("norm", 0) in r:
        for copy in norms:
            copy.wait()
        share = r["norm"].shape[1]
        width = up_to(share + LANES - math.gcd(share, LANES), LANES)
        value = (r["norm"][0:1, :] + r["norm"][1:2, :]).astype(jnp.bfloat16).astype(jnp.float32)
        value = jnp.concatenate([value, jnp.zeros((1, width - share), jnp.float32)], axis=1)
        place = (me * lax.axis_size("model") + lax.axis_index("model")) * share
        value = pltpu.roll(jnp.broadcast_to(value, (GROUP, width)), lax.rem(place, LANES), 1)
        r["lines"][...] = jnp.zeros(r["lines"].shape, jnp.float32)
        for k in range(width // LANES):
            r["lines"][pl.ds(lax.div(place, LANES) + k, 1), :] = value[0:1, k * LANES : (k + 1) * LANES]
        r["gain"][...] = r["lines"][pl.ds(0, r["gain"].shape[0]), :].astype(jnp.bfloat16)
    for p, matrix, at, size in w:
        for first, some in blocks_of(0, size):
            start(
                r["latest_late", p].at[pl.ds(first, some), :],
                r["latest", matrix].at[pl.ds(at + first, some), :],
                r["a_sem", p],
            )
        wait_at_end(r["latest_late", p], r["latest", matrix].at[pl.ds(at, size), :], r["a_sem", p])
    for p, matrix, at, size in [part for part in a if part[0] not in late]:
        wait_at_end(r["latest_out", p], r["latest", matrix].at[pl.ds(at, size), :], r["a_sem", p])
    for copy in wanted.values():
        copy.wait()
    for copy in pending:
        copy.wait()


def local(n, w_gate, first_gate, second_gate, w_up, first_up, second_up, norm_train, norm_step):
    columns, rows = w_gate.shape[1], w_gate.shape[0]
    parts = cut(columns)
    sources = [[x.T for x in (w_gate, first_gate, second_gate)], [x.T for x in (w_up, first_up, second_up)]]
    perms = [[(i, (i + s) % n) for i in range(n)] for s in range(1, n)]
    held = {}
    state = [dict() for _ in parts]
    any_spec = pl.BlockSpec(memory_space=pl.ANY)
    v_spec = pl.BlockSpec(memory_space=pltpu.VMEM)
    stream = stream_of(parts)
    computed = ready = 0

    share = norm_train.shape[0]
    model = lax.axis_size("model")
    lines = n * model * share // LANES
    width = up_to(share + LANES - math.gcd(share, LANES), LANES)
    steps = lambda axis, size: [(axis, [(i, i ^ (1 << k)) for i in range(size)]) for k in range(size.bit_length() - 1)]
    hops = steps("model", model)
    hops[1:1] = steps("zero", n)

    def hop(number):
        for begin, due in HOPS:
            if begin == number and hops:
                axis, perm = hops.pop(0)
                held["near"] = lax.ppermute(held["gain"], axis, perm)
                held["due"] = due

    def stage(number, *lists):
        nonlocal computed, ready
        plan = [[(p, *parts[p]) for p in ps if parts[p][2]] for ps in lists]
        late = [p for stage in STAGES for p in stage[3]]
        ins, outs, scratch, alias = {}, {}, {}, {}
        moved = 0
        latest_spec = (pltpu.HBM((columns, rows), jnp.float32), any_spec)
        ready_spec = (pltpu.HBM((columns, n * rows), jnp.bfloat16), any_spec)
        for p, matrix, at, size in plan[0]:
            if p not in late:
                outs["latest", matrix] = latest_spec
                scratch["a_sem", p] = pltpu.SemaphoreType.DMA
            outs["top_out", p] = (pltpu.VMEM((size, LANES), jnp.float32), v_spec)
            outs["latest_out", p] = (pltpu.VMEM((size, rows), jnp.float32), v_spec)
            moved += 16 * size * rows
        end = computed + sum(1 for block in stream if block[0] in [part[0] for part in plan[0]])
        fetched = (computed, ready, end)
        if end > computed:
            for matrix in sorted({stream[i][1] for i in range(ready, min(end + DEPTH, len(stream)))}):
                for k in range(3):
                    ins["x", matrix, k] = (sources[matrix][k], any_spec)
            if "ring" in held:
                ins["ring_in"] = (held["ring"], v_spec)
                alias["ring_in"] = "ring"
            outs["ring"] = (pltpu.VMEM((DEPTH, 3, BLOCK, rows), jnp.float32), v_spec)
            scratch["in_sem"] = pltpu.SemaphoreType.DMA((DEPTH,))
            computed, ready = end, min(end + DEPTH, len(stream))
        else:
            fetched = (0, len(stream), 0)
        for p, matrix, at, size in plan[1]:
            ins["latest_in", p] = (state[p]["latest"], v_spec)
            ins["top_in", p] = (state[p]["top"], v_spec)
            for s, x in enumerate(state[p]["tops"]):
                ins["top_near", p, s] = (x, v_spec)
            outs["ready", matrix] = ready_spec
            outs["send", p] = (pltpu.VMEM((size, rows), jnp.bfloat16), v_spec)
            if ("column", matrix) in held:
                ins["column_in", matrix] = (held["column", matrix], v_spec)
            space = pltpu.HBM if at + size == columns else pltpu.VMEM
            outs["column", matrix] = (space((columns,), jnp.float32), v_spec)
            most = max(up_to(part[3], LANES) for part in plan[1])
            scratch["column_top"] = pltpu.VMEM((most, LANES), jnp.float32)
            scratch["b_sem", p] = pltpu.SemaphoreType.DMA
            moved += 4 * size * rows
        for p, matrix, at, size in plan[2]:
            for s, x in enumerate(state[p]["arrived"]):
                ins["arrived", p, s] = (x, v_spec)
            if number + 1 < len(STAGES):
                ins["sent", p] = (state[p]["send"], v_spec)
            outs["ready", matrix] = ready_spec
            scratch["c_sem", p] = pltpu.SemaphoreType.DMA((n - 1,))
            moved += 2 * size * rows * (n - 1)
        for p, matrix, at, size in plan[3]:
            ins["latest_late", p] = (state[p]["latest"], v_spec)
            outs["latest", matrix] = latest_spec
            scratch["a_sem", p] = pltpu.SemaphoreType.DMA
            moved += 4 * size * rows
        if "token" in held:
            ins["token_in"] = (held["token"], v_spec)
        if number == 0:
            ins["norm", 0], ins["norm", 1] = (norm_train, any_spec), (norm_step, any_spec)
            outs["gain"] = (pltpu.VMEM((lines, LANES), jnp.bfloat16), v_spec)
            scratch["norm"] = pltpu.VMEM((2, share), jnp.float32)
            scratch["lines"] = pltpu.VMEM((up_to(lines + width // LANES, GROUP), LANES), jnp.float32)
            scratch["norm_sem"] = pltpu.SemaphoreType.DMA((2,))
        if "near" in held and number == held["due"]:
            ins["gain_in"] = (held["gain"], v_spec)
            ins["gain_near"] = (held.pop("near"), v_spec)
            space = pltpu.VMEM if hops else pltpu.HBM
            outs["gain"] = (space((lines, LANES), jnp.bfloat16), v_spec)
        outs["token"] = (pltpu.VMEM((GROUP, LANES), jnp.float32), v_spec)
        for name in outs:
            if name[0] in ("latest", "ready") and name in held:
                ins["in", name] = (held[name], any_spec)
                alias["in", name] = name
        order_in, order_out = list(ins), list(outs)
        results = pl.pallas_call(
            functools.partial(stage_kernel, plan, n, rows, stream, fetched, [*ins, *outs, *scratch]),
            out_shape=[o[0] for o in outs.values()],
            in_specs=[i[1] for i in ins.values()],
            out_specs=[o[1] for o in outs.values()],
            scratch_shapes=list(scratch.values()),
            input_output_aliases={order_in.index(i): order_out.index(o) for i, o in alias.items()},
            cost_estimate=pl.CostEstimate(flops=300 * moved, bytes_accessed=moved, transcendentals=0),
            compiler_params=pltpu.CompilerParams(vmem_limit_bytes=SPARE),
        )(
            *[
                pltpu.with_memory_space_constraint(x, pltpu.VMEM if spec is v_spec else pltpu.HBM)
                for x, spec in ins.values()
            ]
        )
        results = dict(zip(outs, results))
        for name, x in results.items():
            if name[0] in ("latest", "ready", "column") or name in ("token", "ring", "gain"):
                held[name] = x
        for p, matrix, _, _ in plan[0]:
            state[p]["latest"] = results.get(("latest_out", p))
            state[p]["top"] = results["top_out", p]
            state[p]["tops"] = [lax.ppermute(results["top_out", p], "zero", perm) for perm in perms]
        for p, _, _, _ in plan[1]:
            state[p]["send"] = results["send", p]
            state[p]["arrived"] = [lax.ppermute(results["send", p], "zero", perm) for perm in perms]

    for number, lists in enumerate(STAGES):
        stage(number, *lists)
        hop(number)
    while hops:
        axis, perm = hops.pop(0)
        held["gain"] = held["gain"] + lax.ppermute(held["gain"], axis, perm)
    return (
        held["ready", 0].T,
        held["ready", 1].T,
        held["column", 0],
        held["column", 1],
        held["gain"].reshape(-1),
        held["latest", 0].T,
        held["latest", 1].T,
    )


def solution(mesh):
    n = mesh.shape["zero"]
    spec = P("zero", "model")
    specs = dict(
        mesh=mesh,
        in_specs=(spec,) * 6 + (P(("zero", "model")),) * 2,
        out_specs=(P(None, "model"), P(None, "model"), P("model"), P("model"), P(), spec, spec),
        check_vma=False,
    )
    return jax.shard_map(functools.partial(local, n), **specs)
```
